512 devices in a mesh: cyc: 16 (over z), tile: 32 (over x, y, core).
Axes of the slice: x: 4, y: 4, z: 16, core: 2. Of those that a mesh axis runs over, the one named last changes fastest.
Arguments:
- weight_change: bfloat16 [16, 80, 80, 1024], P('cyc', None, None, 'tile'), may hold values from -0.1796875 to 0.1796875
- ensemble: bfloat16 [16, 80, 8, 16384], P('cyc', None, None, 'tile'), may hold values from -6 to 6
- stencil_index: int32 [4, 16384], P(None, 'tile'), may hold values from 0 to 39
- stencil_weight: float32 [4, 16384], P(None, 'tile'), may hold values from 0.1 to 1
Outputs:
- smoothed: bfloat16 [16, 80, 8, 16384], P('cyc', None, None, 'tile')
The draws below stay inside these ranges and needn't reach their ends.
Inputs may be any that keep to these rules, and one draw needn't show every extreme that they name: `stencil_index`: positions 0 to 3 of the extended list are the last columns of the sector before (periodic in longitude), positions 36 and beyond the first columns of the sector after.
All inputs are finite; a program needn't handle non-finite values.
Results may differ from the reference program's by a relative error of at most 0.0085.
Values may be sent and summed in bfloat16 or wider, within the bound.
No kernel may reach another device: no remote copies, remote signals or barrier semaphores. Data moves between devices by JAX's collectives and lax.ppermute only.
A program may use at most 128 MiB of HBM per device.

```python
import jax
import jax.numpy as jnp
from jax import lax

MEMBERS = 80
RIM_COLS = 4
COLS_DEV = 32
FINE_DEV = 512
CYCLES = 16
COLUMNS = 1024
POINTS = 16384
CHANNELS = 8
N_TILE = 32


def with_ends(array, rng, smallest, top_value):
    longest = array.shape.index(max(array.shape))
    spots = []
    for shift in (0, 1):
        where = [jax.random.randint(jax.random.fold_in(rng, axis), (), 0, length) for axis, length in enumerate(array.shape)]
        where[longest] = (where[longest] + shift) % array.shape[longest]
        spots.append(tuple(where))
    return array.at[spots[0]].set(smallest).at[spots[1]].set(top_value)


def steps_of(key, shape, pieces, least, largest):
    gain = 1.0
    for axis_at, blocks in pieces:
        heights = jax.random.uniform(jax.random.fold_in(jax.random.fold_in(key, 6), axis_at), (blocks,), jnp.float32, least / len(pieces), largest / len(pieces))
        gain = gain * jnp.repeat(jnp.exp(heights), shape[axis_at] // blocks).reshape((-1,) + (1,) * (len(shape) - 1 - axis_at))
    return gain


def bell_draw(rng, dims, scale, most, cuts=(), held_as=jnp.bfloat16):
    array = scale * jax.random.normal(rng, dims, jnp.float32)
    if cuts:
        array = array * steps_of(rng, dims, cuts, -0.22, 0.18)
    return jnp.clip(array, -most, most).astype(held_as)


def setup_inputs(seed: int = 0) -> dict:
    streams_of = jax.random.split(jax.random.key(seed), 5)
    return {
        "weight_change": bell_draw(streams_of[0], (CYCLES, MEMBERS, MEMBERS, COLUMNS), 0.03, 0.1796875, ((0, 16), (3, 32))),
        "ensemble": bell_draw(streams_of[1], (CYCLES, MEMBERS, CHANNELS, POINTS), 1.0, 6.0, ((0, 16), (3, 32))),
        "stencil_index": with_ends(jax.random.randint(streams_of[2], (4, POINTS), 0, COLS_DEV + 2 * RIM_COLS), jax.random.fold_in(streams_of[2], 1), 0, (COLS_DEV + 2 * RIM_COLS) - 1).astype(jnp.int32),
        "stencil_weight": jnp.clip(0.1 + 0.9 * jax.random.uniform(streams_of[3], (4, POINTS), jnp.float32) ** steps_of(streams_of[3], (4, POINTS), ((1, 32),), -0.2, 0.2), 0.1, 1.0),
    }


def chain_sector(mats):
    members = mats.shape[1]
    eye = jnp.eye(members, dtype=jnp.float32)[:, :, None]
    start = jnp.broadcast_to(eye, mats.shape[1:])

    def later(carry, weight):
        product = jnp.einsum('ijg,jkg->ikg', weight, carry, precision=lax.Precision.HIGHEST, preferred_element_type=jnp.float32)
        return product, carry

    final, suffix = lax.scan(later, start, mats, reverse=True)
    return suffix


def apply_cycle(inputs, index, shares):
    products, states = inputs
    picked = jnp.take(products, index, axis=2)
    interp = jnp.sum(picked * shares[None, None, :, :], axis=2).astype(jnp.bfloat16)
    mixed = jnp.einsum('nvf,nmf->mvf', states.astype(jnp.float32), interp.astype(jnp.float32), precision=lax.Precision.HIGHEST)
    return mixed.astype(jnp.bfloat16)


def reference(weight_change, ensemble, stencil_index, stencil_weight):
    members = weight_change.shape[1]
    eye = jnp.eye(members, dtype=jnp.float32)[None, :, :, None]
    width = COLS_DEV + 2 * RIM_COLS
    offsets = jnp.arange(width).astype(jnp.int32)

    def sector(tile):
        columns = (tile * COLS_DEV - RIM_COLS + offsets + COLUMNS) % COLUMNS
        raw = jnp.take(weight_change, columns.astype(jnp.int32), axis=3)
        mats = raw.astype(jnp.float32) + eye
        suffix = chain_sector(mats)
        begin = (tile * FINE_DEV).astype(jnp.int32)
        index = lax.dynamic_slice_in_dim(stencil_index, begin, FINE_DEV, 1)
        weights = lax.dynamic_slice_in_dim(stencil_weight, begin, FINE_DEV, 1)
        shares = weights / jnp.sum(weights, axis=0, keepdims=True)
        states = lax.dynamic_slice_in_dim(ensemble, begin, FINE_DEV, 3)
        return lax.map(lambda pair: apply_cycle(pair, index, shares), (suffix, states))

    tiles = jnp.arange(N_TILE).astype(jnp.int32)
    result = lax.map(sector, tiles)
    result = jnp.moveaxis(result, 0, 3)
    return result.reshape(CYCLES, members, CHANNELS, N_TILE * FINE_DEV)
```

```python
import jax
import jax.numpy as jnp
from jax import lax
from jax.experimental import pallas as pl
from jax.experimental.pallas import tpu as pltpu
from jax.sharding import PartitionSpec as P

RIM = 4
LANES = 128
SPAN = 4
NEAR = [[SPAN * k + r for r in range(SPAN)] for k in range(SPAN)]
FAR = [[SPAN * k + r for k in range(SPAN)] for r in range(SPAN)]
F32 = jnp.float32
BF16 = jnp.bfloat16


def mm(a, b):
    return jnp.dot(a, b, preferred_element_type=F32)


def mm_split(a, b):
    high = a.astype(BF16)
    low = (a - high.astype(F32)).astype(BF16)
    return mm(high, b) + mm(low, b)


def part(array, g, n):
    return array[:, g * n : (g + 1) * n]


def pack_kernel(x_ref, out_ref, rows):
    n, cols, _ = x_ref.shape
    per = cols // SPAN
    for i in range(n):
        rows[i * cols : (i + 1) * cols, :n] = x_ref[i].astype(F32)
    for q in range(SPAN):
        mats = [rows[pl.ds(q * per + g, n, stride=cols), :].T[:n] for g in range(per)]
        out_ref[q] = jnp.concatenate(mats, axis=1).astype(BF16)


def near_kernel(d_ref, e_ref, g_ref):
    n = d_ref.shape[1]
    per = d_ref.shape[2] // n
    d = [d_ref[r] for r in range(SPAN)]
    e0s, e1s, gs = [], [], []
    for g in range(per):
        d0, d1, d2, d3 = [part(a, g, n) for a in d]
        e1 = d3.astype(F32) + d2.astype(F32) + mm(d3, d2)
        e0 = e1 + d1.astype(F32) + mm_split(e1, d1)
        whole = e0 + d0.astype(F32) + mm_split(e0, d0)
        e0s.append(e0)
        e1s.append(e1)
        gs.append(whole)
    e_ref[0] = jnp.concatenate(e0s, axis=1)
    e_ref[1] = jnp.concatenate(e1s, axis=1)
    e_ref[2] = d[3].astype(F32)
    g_ref[...] = jnp.concatenate(gs, axis=1).astype(BF16)


def far_kernel(mine_ref, w_ref, e_ref, out_ref):
    n = w_ref.shape[1]
    per = w_ref.shape[2] // n
    mine = mine_ref[0]
    h = [w_ref[k] * jnp.where(mine < k, 1.0, 0.0).astype(BF16) for k in range(SPAN)]
    e = [e_ref[r] for r in range(SPAN - 1)]
    outs = [[] for _ in range(SPAN)]
    for g in range(per):
        _, h1, h2, h3 = [part(a, g, n) for a in h]
        s = h3.astype(F32) + h2.astype(F32) + mm(h3, h2)
        s = s + h1.astype(F32) + mm_split(s, h1)
        for r in range(SPAN - 1):
            er = part(e[r], g, n)
            outs[r].append(s + er + mm_split(s, er.astype(BF16)))
        outs[SPAN - 1].append(s)
    for r in range(SPAN):
        out_ref[r] = jnp.concatenate(outs[r], axis=1).astype(BF16)


def table_of(index_ref, weight_ref, slots):
    weight = weight_ref[...]
    share = weight / jnp.sum(weight, axis=0, keepdims=True)
    index = index_ref[...]
    points = index.shape[1]
    row = lax.broadcasted_iota(jnp.int32, (slots, points), 0)
    table = jnp.zeros((slots, points), F32)
    for j in range(4):
        table = table + jnp.where(index[j][None, :] == row, share[j][None, :], 0.0)
    return table


def apply_kernel(index_ref, weight_ref, x_ref, p_ref, low_ref, high_ref, out_ref, rows, tall):
    n, channels, points = x_ref.shape
    chunks = p_ref.shape[0]
    per = p_ref.shape[2] // n
    slots = chunks * per + 2 * RIM
    wide = points // LANES
    for i in range(n):
        for t in range(wide):
            rows[t, i * channels : (i + 1) * channels, :] = x_ref[i, :, t * LANES : (t + 1) * LANES].astype(F32)
    table = table_of(index_ref, weight_ref, slots)
    for g in range(slots):
        tall[g] = jnp.broadcast_to(table[g][None, :], (16, points)).astype(BF16)

    def channel(v, carry):
        at = pl.ds(v, n, stride=channels)
        state = jnp.concatenate([rows[t, at, :] for t in range(wide)], axis=1)
        x = state.astype(BF16).reshape(n // 16, 16, points)

        def scaled(slot):
            return (x * tall[slot][None]).reshape(n, points)

        acc = state
        for i in range(chunks):
            many = jnp.concatenate([scaled(RIM + i * per + g) for g in range(per)], axis=0)
            acc = acc + mm(p_ref[i], many)
        many = jnp.concatenate([scaled(g) for g in range(RIM)], axis=0)
        acc = acc + mm(low_ref[...], many)
        many = jnp.concatenate([scaled(RIM + chunks * per + g) for g in range(RIM)], axis=0)
        acc = acc + mm(high_ref[...], many)
        for t in range(wide):
            rows[t, at, :] = acc[:, t * LANES : (t + 1) * LANES]
        return carry

    lax.fori_loop(0, channels, channel, 0)
    for i in range(n):
        for t in range(wide):
            out_ref[i, :, t * LANES : (t + 1) * LANES] = rows[t, i * channels : (i + 1) * channels, :].astype(BF16)


def call(body, outs, scratch=(), inputs=0, scalars=0, name=None):
    vmem = pl.BlockSpec(memory_space=pltpu.VMEM)
    smem = pl.BlockSpec(memory_space=pltpu.SMEM)
    return pl.pallas_call(
        body,
        out_shape=outs,
        in_specs=[smem] * scalars + [vmem] * inputs,
        out_specs=jax.tree.map(lambda _: vmem, outs),
        scratch_shapes=list(scratch),
        compiler_params=pltpu.CompilerParams(vmem_limit_bytes=56 * 1024 * 1024),
        name=name,
    )


def on_device(weight_change, ensemble, stencil_index, stencil_weight):
    _, n, _, cols = weight_change.shape
    per = cols // SPAN
    lanes = per * n
    chunk = jax.ShapeDtypeStruct((SPAN, n, lanes), BF16)
    raw = jnp.transpose(weight_change[0], (0, 2, 1))
    states = ensemble[0]
    points = states.shape[2]

    packed = call(pack_kernel, chunk, [pltpu.VMEM((n * cols, LANES), F32)], inputs=1, name="pack")(raw)
    mine = lax.all_to_all(packed, "cyc", 0, 0, axis_index_groups=NEAR, tiled=True)
    near, whole = call(
        near_kernel,
        (jax.ShapeDtypeStruct((SPAN - 1, n, lanes), F32), jax.ShapeDtypeStruct((n, lanes), BF16)),
        inputs=1,
        name="near",
    )(mine)
    wholes = lax.all_gather(whole, "cyc", axis=0, axis_index_groups=FAR)
    group = (lax.axis_index("cyc") // SPAN).astype(jnp.int32).reshape(1)
    sent = call(far_kernel, chunk, inputs=2, scalars=1, name="far")(group, wholes, near)
    suffix = lax.all_to_all(sent, "cyc", 0, 0, axis_index_groups=NEAR, tiled=True)

    count = lax.axis_size("tile")
    forward = [(i, (i + 1) % count) for i in range(count)]
    backward = [(target, source) for source, target in forward]
    low = lax.ppermute(suffix[SPAN - 1, :, lanes - RIM * n :], "tile", forward)
    high = lax.ppermute(suffix[0, :, : RIM * n], "tile", backward)
    slots = cols + 2 * RIM
    result = call(
        apply_kernel,
        jax.ShapeDtypeStruct(states.shape, BF16),
        [pltpu.VMEM((points // LANES, n * states.shape[1], LANES), F32), pltpu.VMEM((slots, 16, points), BF16)],
        inputs=6,
        name="apply",
    )(stencil_index, stencil_weight, states, suffix, low, high)
    return result[None]


def solution(mesh):
    placed = (
        P("cyc", None, None, "tile"),
        P("cyc", None, None, "tile"),
        P(None, "tile"),
        P(None, "tile"),
    )
    return jax.shard_map(
        on_device,
        mesh=mesh,
        in_specs=placed,
        out_specs=P("cyc", None, None, "tile"),
        check_vma=False,
    )
```

```python
import jax
import jax.numpy as jnp
from jax import lax
from jax.experimental import pallas as pl
from jax.experimental.pallas import tpu as pltpu
from jax.sharding import PartitionSpec as P

RIM = 4
LANES = 128
SPAN = 4
NEAR = [[SPAN * k + r for r in range(SPAN)] for k in range(SPAN)]
FAR = [[SPAN * k + r for k in range(SPAN)] for r in range(SPAN)]
F32 = jnp.float32
BF16 = jnp.bfloat16


def mm(a, b):
    return jnp.dot(a, b, preferred_element_type=F32)


def halves(a):
    high = a.astype(BF16)
    low = (a - high.astype(F32)).astype(BF16)
    return jnp.concatenate([high, low], axis=0)


def product(a, b):
    n, lanes = b.shape
    block = lax.broadcasted_iota(jnp.int32, (1, lanes), 1) // n
    rows = [jnp.where(block == g, b, jnp.zeros_like(b)) for g in range(lanes // n)]
    square = jnp.concatenate(rows, axis=0)
    outs = []
    for begin in range(0, lanes, 2 * LANES):
        end = min(lanes, begin + 2 * LANES)
        first = begin // n * n // LANES * LANES
        last = min(lanes, -(-(-(-end // n) * n) // LANES) * LANES)
        outs.append(mm(a[:, first:last], square[first:last, begin:end]))
    return jnp.concatenate(outs, axis=1)


def joined(a, b):
    n = b.shape[0]
    both = product(halves(a), b)
    return a + b.astype(F32) + both[:n] + both[n:]


def pack_kernel(x_ref, out_ref, rows):
    n, cols, _ = x_ref.shape
    per = cols // SPAN
    for i in range(n):
        rows[i * cols : (i + 1) * cols, :n] = x_ref[i].astype(F32)
    for q in range(SPAN):
        mats = [rows[pl.ds(q * per + g, n, stride=cols), :].T[:n] for g in range(per)]
        out_ref[q] = jnp.concatenate(mats, axis=1).astype(BF16)


def near_kernel(d_ref, e_ref, g_ref):
    d0, d1, d2, d3 = [d_ref[r] for r in range(SPAN)]
    e1 = d3.astype(F32) + d2.astype(F32) + product(d3, d2)
    e0 = joined(e1, d1)
    e_ref[0] = e0.astype(BF16)
    e_ref[1] = e1.astype(BF16)
    e_ref[2] = d3
    g_ref[...] = joined(e0, d0).astype(BF16)


def far_kernel(mine_ref, w_ref, e_ref, out_ref, own_ref, made, sems):
    mine = mine_ref[0]
    place = mine_ref[1]
    _, h1, h2, h3 = [w_ref[k] * jnp.where(mine < k, 1.0, 0.0).astype(BF16) for k in range(SPAN)]
    s = joined(h3.astype(F32) + h2.astype(F32) + product(h3, h2), h1)
    n = s.shape[0]
    parts = halves(s)
    copies = [pltpu.make_async_copy(made.at[r], out_ref.at[r], sems.at[r]) for r in range(SPAN)]
    made[SPAN - 1] = s.astype(BF16)
    copies[SPAN - 1].start()
    for r in range(SPAN - 1):
        e = e_ref[r]
        both = product(parts, e)
        made[r] = (s + e.astype(F32) + both[:n] + both[n:]).astype(BF16)
        copies[r].start()
    own_ref[...] = made[place]
    for copy in copies:
        copy.wait()


def table_of(index_ref, weight_ref, slots):
    weight = weight_ref[...]
    share = weight / jnp.sum(weight, axis=0, keepdims=True)
    index = index_ref[...]
    points = index.shape[1]
    row = lax.broadcasted_iota(jnp.int32, (slots, points), 0)
    table = jnp.zeros((slots, points), F32)
    for j in range(4):
        table = table + jnp.where(index[j][None, :] == row, share[j][None, :], 0.0)
    return table


def ready_kernel(index_ref, weight_ref, x_ref, states_ref, tall_ref, rows):
    n, channels, points = x_ref.shape
    wide = points // LANES
    for i in range(n):
        for t in range(wide):
            rows[t, i * channels : (i + 1) * channels, :] = x_ref[i, :, t * LANES : (t + 1) * LANES].astype(F32)
    for v in range(channels):
        for t in range(wide):
            states_ref[v, :, t * LANES : (t + 1) * LANES] = rows[t, pl.ds(v, n, stride=channels), :].astype(BF16)
    slots = tall_ref.shape[0]
    table = table_of(index_ref, weight_ref, slots)
    for g in range(slots):
        tall_ref[g] = jnp.broadcast_to(table[g][None, :], (16, points)).astype(BF16)


def mixed(states_ref, tall_ref, v, matrices, slots, begin=0, points=None):
    _, n, whole = states_ref.shape
    points = points or whole
    at = slice(begin, begin + points)
    x = states_ref[v, :, at].reshape(n // 16, 16, points)
    many = jnp.concatenate([(x * tall_ref[slot, :, at][None]).reshape(n, points) for slot in slots], axis=0)
    return mm(matrices, many)


def own_kernel(mine_ref, p_ref, states_ref, tall_ref, out_ref):
    channels, n, _ = states_ref.shape
    per = p_ref.shape[1] // n
    begin = RIM + mine_ref[1] * per
    p = p_ref[...]
    for v in range(channels):
        out_ref[v] = states_ref[v].astype(F32) + mixed(states_ref, tall_ref, v, p, [begin + g for g in range(per)])


def rest_kernel(mine_ref, p_ref, states_ref, tall_ref, acc_ref, out_ref):
    channels, n, _ = states_ref.shape
    per = p_ref.shape[2] // n
    order = [lax.rem(mine_ref[1] + d, SPAN) for d in range(1, SPAN)]
    p = jnp.concatenate([p_ref[i] for i in order], axis=1)
    slots = [RIM + i * per + g for i in order for g in range(per)]
    for v in range(channels):
        out_ref[v] = acc_ref[v] + mixed(states_ref, tall_ref, v, p, slots)


def halo_kernel(odd_ref, mate_ref, other_ref, states_ref, tall_ref, acc_ref, out_ref, rows, made, sems):
    channels, n, points = states_ref.shape
    last = tall_ref.shape[0]
    slots = [*range(RIM), *range(last - RIM, last)]
    odd = odd_ref[0] == 1
    low = jnp.where(odd, mate_ref[...], other_ref[...])
    high = jnp.where(odd, other_ref[...], mate_ref[...])
    p = jnp.concatenate([low, high], axis=1)
    copies = []
    for begin in range(0, points, 2 * LANES):
        for v in range(channels):
            acc = acc_ref[v, :, begin : begin + 2 * LANES]
            acc = acc + mixed(states_ref, tall_ref, v, p, slots, begin, 2 * LANES)
            for t in range(2):
                rows[t, pl.ds(v, n, stride=channels), :] = acc[:, t * LANES : (t + 1) * LANES]
        for t in range(2):
            at = slice(begin + t * LANES, begin + (t + 1) * LANES)
            for i in range(n):
                made[i, :, at] = rows[t, i * channels : (i + 1) * channels, :].astype(BF16)
        at = pl.ds(begin, 2 * LANES)
        copy = pltpu.make_async_copy(made.at[:, :, at], out_ref.at[:, :, at], sems.at[len(copies)])
        copy.start()
        copies.append(copy)
    for copy in copies:
        copy.wait()


def call(body, outs, *operands, scratch=(), scalars=0, flops=None):
    vmem = pl.BlockSpec(memory_space=pltpu.VMEM)
    smem = pl.BlockSpec(memory_space=pltpu.SMEM)
    held = [
        x[0] if isinstance(x, tuple) else pltpu.with_memory_space_constraint(x, pltpu.VMEM) for x in operands[scalars:]
    ]
    cost = None if flops is None else pl.CostEstimate(flops=flops, bytes_accessed=0, transcendentals=0)
    return pl.pallas_call(
        body,
        out_shape=outs,
        in_specs=[smem] * scalars + [vmem] * len(held),
        out_specs=jax.tree.map(
            lambda out: pl.BlockSpec(memory_space=pltpu.HBM) if isinstance(out, jax.ShapeDtypeStruct) else vmem,
            outs,
            is_leaf=lambda x: not isinstance(x, (list, tuple)),
        ),
        scratch_shapes=list(scratch),
        compiler_params=pltpu.CompilerParams(vmem_limit_bytes=40 * 1024 * 1024),
        cost_estimate=cost,
        name=body.__name__.removesuffix("_kernel"),
    )(*operands[:scalars], *held)


def on_device(weight_change, ensemble, stencil_index, stencil_weight):
    _, n, _, cols = weight_change.shape
    per = cols // SPAN
    lanes = per * n
    shape = jax.ShapeDtypeStruct
    raw = jnp.transpose(weight_change[0], (0, 2, 1))
    states = ensemble[0]
    _, channels, points = states.shape
    slots = cols + 2 * RIM
    rows = pltpu.VMEM((points // LANES, n * channels, LANES), F32)

    chunk = pltpu.VMEM((n, lanes), BF16)
    chunks = pltpu.VMEM((SPAN, n, lanes), BF16)
    packed = call(pack_kernel, chunks, (raw,), scratch=[pltpu.VMEM((n * cols, LANES), F32)])
    days = lax.all_to_all(packed, "cyc", 0, 0, axis_index_groups=NEAR, tiled=True)
    flat, tall = call(
        ready_kernel,
        (pltpu.VMEM((channels, n, points), BF16), pltpu.VMEM((slots, 16, points), BF16)),
        (stencil_index,),
        (stencil_weight,),
        (states,),
        scratch=[rows],
        flops=400_000_000,
    )
    near, whole = call(near_kernel, (pltpu.VMEM((SPAN - 1, n, lanes), BF16), chunk), days)
    wholes = lax.all_gather(whole, "cyc", axis=0, axis_index_groups=FAR)
    place = lax.axis_index("cyc").astype(jnp.int32)
    mine = jnp.stack([place // SPAN, place % SPAN])
    sent, own = call(
        far_kernel,
        (shape((SPAN, n, lanes), BF16), chunk),
        mine,
        wholes,
        near,
        scratch=[chunks, pltpu.SemaphoreType.DMA((SPAN,))],
        scalars=1,
    )
    suffix = lax.all_to_all(sent, "cyc", 0, 0, axis_index_groups=NEAR, tiled=True)
    count = lax.axis_size("tile")
    odd = lax.axis_index("tile").astype(jnp.int32) % 2
    first, last = suffix[0, :, : RIM * n], suffix[SPAN - 1, :, lanes - RIM * n :]
    others = [(i, (i - 1 + 2 * (i % 2)) % count) for i in range(count)]
    mates = [(i, i + 1 - 2 * (i % 2)) for i in range(count)]
    other = lax.ppermute(jnp.where(odd == 1, last, first), "tile", others)
    mate = lax.ppermute(jnp.where(odd == 1, first, last), "tile", mates)
    sums = pltpu.VMEM((channels, n, points), F32)
    acc = call(own_kernel, sums, mine, own, flat, tall, scalars=1, flops=420_000_000)
    acc = call(rest_kernel, sums, mine, suffix, flat, tall, acc, scalars=1, flops=1_260_000_000)
    result = call(
        halo_kernel,
        shape(states.shape, BF16),
        odd.reshape(1),
        mate,
        other,
        flat,
        tall,
        acc,
        scratch=[
            pltpu.VMEM((2, n * channels, LANES), F32),
            pltpu.VMEM(states.shape, BF16),
            pltpu.SemaphoreType.DMA((points // LANES // 2,)),
        ],
        scalars=1,
    )
    return result[None]


def solution(mesh):
    placed = (
        P("cyc", None, None, "tile"),
        P("cyc", None, None, "tile"),
        P(None, "tile"),
        P(None, "tile"),
    )
    return jax.shard_map(
        on_device,
        mesh=mesh,
        in_specs=placed,
        out_specs=P("cyc", None, None, "tile"),
        check_vma=False,
    )
```

```python
import jax
import jax.numpy as jnp
from jax import lax
from jax.experimental import pallas as pl
from jax.experimental.pallas import tpu as pltpu
from jax.sharding import PartitionSpec as P

RIM = 4
LANES = 128
SPAN = 4
NEAR = [[SPAN * k + r for r in range(SPAN)] for k in range(SPAN)]
FAR = [[SPAN * k + r for k in range(SPAN)] for r in range(SPAN)]
F32 = jnp.float32
BF16 = jnp.bfloat16


def mm(a, b):
    return jnp.dot(a, b, preferred_element_type=F32)


def halves(a):
    high = a.astype(BF16)
    low = (a - high.astype(F32)).astype(BF16)
    return jnp.concatenate([high, low], axis=0)


def product(a, b):
    n, lanes = b.shape
    block = lax.broadcasted_iota(jnp.int32, (1, lanes), 1) // n
    rows = [jnp.where(block == g, b, jnp.zeros_like(b)) for g in range(lanes // n)]
    square = jnp.concatenate(rows, axis=0)
    outs = []
    for begin in range(0, lanes, 2 * LANES):
        end = min(lanes, begin + 2 * LANES)
        first = begin // n * n // LANES * LANES
        last = min(lanes, -(-(-(-end // n) * n) // LANES) * LANES)
        outs.append(mm(a[:, first:last], square[first:last, begin:end]))
    return jnp.concatenate(outs, axis=1)


def joined(a, b):
    n = b.shape[0]
    both = product(halves(a), b)
    return a + b.astype(F32) + both[:n] + both[n:]


def pack_kernel(x_ref, out_ref, rows):
    n, cols, _ = x_ref.shape
    per = cols // SPAN
    for i in range(n):
        rows[i * cols : (i + 1) * cols, :n] = x_ref[i].astype(F32)
    for q in range(SPAN):
        mats = [rows[pl.ds(q * per + g, n, stride=cols), :].T[:n] for g in range(per)]
        out_ref[q] = jnp.concatenate(mats, axis=1).astype(BF16)


def near_kernel(d_ref, e_ref, g_ref):
    d0, d1, d2, d3 = [d_ref[r] for r in range(SPAN)]
    e1 = d3.astype(F32) + d2.astype(F32) + product(d3, d2)
    e0 = joined(e1, d1)
    e_ref[0] = e0.astype(BF16)
    e_ref[1] = e1.astype(BF16)
    e_ref[2] = d3
    g_ref[...] = joined(e0, d0).astype(BF16)


def far_kernel(mine_ref, w_ref, e_ref, out_ref):
    mine = mine_ref[0]
    _, h1, h2, h3 = [w_ref[k] * jnp.where(mine < k, 1.0, 0.0).astype(BF16) for k in range(SPAN)]
    s = joined(h3.astype(F32) + h2.astype(F32) + product(h3, h2), h1)
    n = s.shape[0]
    parts = halves(s)
    out_ref[SPAN - 1] = s.astype(BF16)
    for r in range(SPAN - 1):
        e = e_ref[r]
        both = product(parts, e)
        out_ref[r] = (s + e.astype(F32) + both[:n] + both[n:]).astype(BF16)


def table_of(index_ref, weight_ref, slots):
    weight = weight_ref[...]
    share = weight / jnp.sum(weight, axis=0, keepdims=True)
    index = index_ref[...]
    points = index.shape[1]
    row = lax.broadcasted_iota(jnp.int32, (slots, points), 0)
    table = jnp.zeros((slots, points), F32)
    for j in range(4):
        table = table + jnp.where(index[j][None, :] == row, share[j][None, :], 0.0)
    return table


def ready_kernel(index_ref, weight_ref, x_ref, states_ref, tall_ref, rows):
    n, channels, points = x_ref.shape
    wide = points // LANES
    for i in range(n):
        for t in range(wide):
            rows[t, i * channels : (i + 1) * channels, :] = x_ref[i, :, t * LANES : (t + 1) * LANES].astype(F32)
    for v in range(channels):
        for t in range(wide):
            states_ref[v, :, t * LANES : (t + 1) * LANES] = rows[t, pl.ds(v, n, stride=channels), :].astype(BF16)
    slots = tall_ref.shape[0]
    table = table_of(index_ref, weight_ref, slots)
    for g in range(slots):
        tall_ref[g] = jnp.broadcast_to(table[g][None, :], (16, points)).astype(BF16)


def mixed(states_ref, tall_ref, v, matrices, slots, begin=0, points=None):
    _, n, whole = states_ref.shape
    points = points or whole
    at = slice(begin, begin + points)
    x = states_ref[v, :, at].reshape(n // 16, 16, points)
    many = jnp.concatenate([(x * tall_ref[slot, :, at][None]).reshape(n, points) for slot in slots], axis=0)
    return mm(matrices, many)


def local_kernel(p_ref, states_ref, tall_ref, out_ref):
    channels, n, _ = states_ref.shape
    chunks = p_ref.shape[0]
    slots = range(RIM, RIM + chunks * (p_ref.shape[2] // n))
    p = jnp.concatenate([p_ref[i] for i in range(chunks)], axis=1)
    for v in range(channels):
        out_ref[v] = states_ref[v].astype(F32) + mixed(states_ref, tall_ref, v, p, slots)


def halo_kernel(odd_ref, mate_ref, other_ref, states_ref, tall_ref, acc_ref, out_ref, rows, made, sems):
    channels, n, points = states_ref.shape
    last = tall_ref.shape[0]
    slots = [*range(RIM), *range(last - RIM, last)]
    odd = odd_ref[0] == 1
    low = jnp.where(odd, mate_ref[...], other_ref[...])
    high = jnp.where(odd, other_ref[...], mate_ref[...])
    p = jnp.concatenate([low, high], axis=1)
    copies = []
    for begin in range(0, points, 2 * LANES):
        for v in range(channels):
            acc = acc_ref[v, :, begin : begin + 2 * LANES]
            acc = acc + mixed(states_ref, tall_ref, v, p, slots, begin, 2 * LANES)
            for t in range(2):
                rows[t, pl.ds(v, n, stride=channels), :] = acc[:, t * LANES : (t + 1) * LANES]
        for t in range(2):
            at = slice(begin + t * LANES, begin + (t + 1) * LANES)
            for i in range(n):
                made[i, :, at] = rows[t, i * channels : (i + 1) * channels, :].astype(BF16)
        at = pl.ds(begin, 2 * LANES)
        copy = pltpu.make_async_copy(made.at[:, :, at], out_ref.at[:, :, at], sems.at[len(copies)])
        copy.start()
        copies.append(copy)
    for copy in copies:
        copy.wait()


def call(body, outs, *operands, scratch=(), scalars=0, flops=None):
    vmem = pl.BlockSpec(memory_space=pltpu.VMEM)
    smem = pl.BlockSpec(memory_space=pltpu.SMEM)
    held = [
        x[0] if isinstance(x, tuple) else pltpu.with_memory_space_constraint(x, pltpu.VMEM) for x in operands[scalars:]
    ]
    cost = None if flops is None else pl.CostEstimate(flops=flops, bytes_accessed=0, transcendentals=0)
    return pl.pallas_call(
        body,
        out_shape=outs,
        in_specs=[smem] * scalars + [vmem] * len(held),
        out_specs=jax.tree.map(
            lambda out: pl.BlockSpec(memory_space=pltpu.HBM) if isinstance(out, jax.ShapeDtypeStruct) else vmem,
            outs,
            is_leaf=lambda x: not isinstance(x, (list, tuple)),
        ),
        scratch_shapes=list(scratch),
        compiler_params=pltpu.CompilerParams(vmem_limit_bytes=40 * 1024 * 1024),
        cost_estimate=cost,
        name=body.__name__.removesuffix("_kernel"),
    )(*operands[:scalars], *held)


def on_device(weight_change, ensemble, stencil_index, stencil_weight):
    _, n, _, cols = weight_change.shape
    per = cols // SPAN
    lanes = per * n
    shape = jax.ShapeDtypeStruct
    raw = jnp.transpose(weight_change[0], (0, 2, 1))
    states = ensemble[0]
    _, channels, points = states.shape
    slots = cols + 2 * RIM
    rows = pltpu.VMEM((points // LANES, n * channels, LANES), F32)

    chunk = pltpu.VMEM((n, lanes), BF16)
    chunks = pltpu.VMEM((SPAN, n, lanes), BF16)
    place = lax.axis_index("cyc").astype(jnp.int32)
    sector = lax.axis_index("tile").astype(jnp.int32)
    mine = jnp.stack([place // SPAN, place % SPAN])
    raw, mine, odd, is_odd = lax.optimization_barrier((raw, mine, (sector % 2).reshape(1), sector % 2 == 1))
    packed = call(pack_kernel, chunks, (raw,), scratch=[pltpu.VMEM((n * cols, LANES), F32)])
    days = lax.all_to_all(packed, "cyc", 0, 0, axis_index_groups=NEAR, tiled=True)
    flat, tall = call(
        ready_kernel,
        (pltpu.VMEM((channels, n, points), BF16), pltpu.VMEM((slots, 16, points), BF16)),
        (stencil_index,),
        (stencil_weight,),
        (states,),
        scratch=[rows],
        flops=400_000_000,
    )
    days, flat, tall = lax.optimization_barrier((days, flat, tall))
    near, whole = call(near_kernel, (pltpu.VMEM((SPAN - 1, n, lanes), BF16), chunk), days)
    wholes = lax.all_gather(whole, "cyc", axis=0, axis_index_groups=FAR)
    sent = call(far_kernel, chunks, mine, wholes, near, scalars=1)
    suffix = lax.all_to_all(sent, "cyc", 0, 0, axis_index_groups=NEAR, tiled=True)
    count = lax.axis_size("tile")
    first, last = suffix[0, :, : RIM * n], suffix[SPAN - 1, :, lanes - RIM * n :]
    others = [(i, (i - 1 + 2 * (i % 2)) % count) for i in range(count)]
    mates = [(i, i + 1 - 2 * (i % 2)) for i in range(count)]
    other = lax.ppermute(jnp.where(is_odd, last, first), "tile", others)
    mate = lax.ppermute(jnp.where(is_odd, first, last), "tile", mates)
    sums = pltpu.VMEM((channels, n, points), F32)
    acc = call(local_kernel, sums, suffix, flat, tall, flops=1_680_000_000)
    result = call(
        halo_kernel,
        shape(states.shape, BF16),
        odd,
        mate,
        other,
        flat,
        tall,
        acc,
        scratch=[
            pltpu.VMEM((2, n * channels, LANES), F32),
            pltpu.VMEM(states.shape, BF16),
            pltpu.SemaphoreType.DMA((points // LANES // 2,)),
        ],
        scalars=1,
    )
    return result[None]


def solution(mesh):
    placed = (
        P("cyc", None, None, "tile"),
        P("cyc", None, None, "tile"),
        P(None, "tile"),
        P(None, "tile"),
    )
    return jax.shard_map(
        on_device,
        mesh=mesh,
        in_specs=placed,
        out_specs=P("cyc", None, None, "tile"),
        check_vma=False,
    )
```
